32 devices in a mesh: dp: 4 (over y, z), sp: 8 (over x, core).
Axes of the slice: x: 4, y: 2, z: 2, core: 2. Of those that a mesh axis runs over, the one named last changes fastest.
The devices are a block of a 4x4x8 slice.
Arguments:
- x: bfloat16 [64, 1536, 512], P('dp', 'sp'), parts along dimension 0
- ln1_gain: bfloat16 [512], replicated
- ln1_bias: bfloat16 [512], replicated
- w_query: bfloat16 [512, 512], replicated
- b_query: bfloat16 [512], replicated
- w_key: bfloat16 [512, 512], replicated
- w_value: bfloat16 [512, 512], replicated
- b_value: bfloat16 [512], replicated
- w_out: bfloat16 [512, 512], replicated
- b_out: bfloat16 [512], replicated
- ln2_gain: bfloat16 [512], replicated
- ln2_bias: bfloat16 [512], replicated
- w_up: bfloat16 [512, 2048], replicated
- b_up: bfloat16 [2048], replicated
- w_down: bfloat16 [2048, 512], replicated
- b_down: bfloat16 [512], replicated
- lnp_gain: bfloat16 [512], replicated
- lnp_bias: bfloat16 [512], replicated
- cross_wk: bfloat16 [6, 512, 512], P(None, None, 'sp')
- cross_wv: bfloat16 [6, 512, 512], P(None, None, 'sp')
- cross_bv: bfloat16 [6, 512], P(None, 'sp')
Outputs:
- output 1: bfloat16 [6, 64, 1536, 8, 64], P(None, 'dp', None, 'sp'), parts along dimension 1
- output 2: bfloat16 [6, 64, 1536, 8, 64], P(None, 'dp', None, 'sp'), parts along dimension 1
There are 4 independent parts. The reference program is written for one: setup_inputs(seed, part) draws one part's arguments, and reference() takes and returns one part's arrays. A program takes and returns all parts, laid end to end along the dimension named above; an argument that names none is the same for every part.
All inputs are finite; a program needn't handle non-finite values.
Results may differ from the reference program's by a relative error of at most 0.00610293.
Values are sent between devices in bfloat16 or wider.
A program may use at most 768 MiB of HBM per device.

```python
import math
import jax
import jax.numpy as jnp
from jax import lax

BATCH_SIZE = 16
FRAMES = 1536
D_MODEL = 512
NUM_HEADS = 8
FF_DIM = 2048
DEC_LAYERS = 6
HEAD_DIM = D_MODEL // NUM_HEADS


def normal_draw(rng_key, dims, std_dev):
    return (jax.random.normal(rng_key, dims, jnp.float32) * std_dev).astype(jnp.bfloat16)


def gain_draw(rng_key, width):
    return (1.0 + 0.2 * jax.random.normal(rng_key, (width,), jnp.float32)).astype(jnp.bfloat16)


def setup_inputs(seed: int = 0, part: int = 0) -> dict:
    base_key = jax.random.key(seed)
    part_key = jax.random.fold_in(base_key, part)
    key_list = jax.random.split(base_key, 20)
    score_std = math.sqrt(math.log(FRAMES / 4.0))
    qk_std = math.sqrt(score_std / D_MODEL)
    out_std = D_MODEL ** -0.5
    return {
        'x': normal_draw(part_key, (BATCH_SIZE, FRAMES, D_MODEL), 1.0),
        'ln1_gain': gain_draw(key_list[0], D_MODEL),
        'ln1_bias': normal_draw(key_list[1], (D_MODEL,), 0.2),
        'w_query': normal_draw(key_list[2], (D_MODEL, D_MODEL), qk_std),
        'b_query': normal_draw(key_list[3], (D_MODEL,), 0.5 * math.sqrt(score_std)),
        'w_key': normal_draw(key_list[4], (D_MODEL, D_MODEL), qk_std),
        'w_value': normal_draw(key_list[5], (D_MODEL, D_MODEL), out_std),
        'b_value': normal_draw(key_list[6], (D_MODEL,), 0.5),
        'w_out': normal_draw(key_list[7], (D_MODEL, D_MODEL), out_std),
        'b_out': normal_draw(key_list[8], (D_MODEL,), 0.3),
        'ln2_gain': gain_draw(key_list[9], D_MODEL),
        'ln2_bias': normal_draw(key_list[10], (D_MODEL,), 0.2),
        'w_up': normal_draw(key_list[11], (D_MODEL, FF_DIM), out_std),
        'b_up': normal_draw(key_list[12], (FF_DIM,), 0.5),
        'w_down': normal_draw(key_list[13], (FF_DIM, D_MODEL), FF_DIM ** -0.5),
        'b_down': normal_draw(key_list[14], (D_MODEL,), 0.3),
        'lnp_gain': gain_draw(key_list[15], D_MODEL),
        'lnp_bias': normal_draw(key_list[16], (D_MODEL,), 0.2),
        'cross_wk': normal_draw(key_list[17], (DEC_LAYERS, D_MODEL, D_MODEL), out_std),
        'cross_wv': normal_draw(key_list[18], (DEC_LAYERS, D_MODEL, D_MODEL), out_std),
        'cross_bv': normal_draw(key_list[19], (DEC_LAYERS, D_MODEL), 0.5),
    }


def layer_norm(hidden_in, ln_gain, ln_bias):
    mean_val = jnp.mean(hidden_in, axis=-1, keepdims=True)
    centered = hidden_in - mean_val
    variance = jnp.mean(centered * centered, axis=-1, keepdims=True)
    return centered * lax.rsqrt(variance + 1e-5) * ln_gain.astype(jnp.float32) + ln_bias.astype(jnp.float32)


def reference(x, ln1_gain, ln1_bias, w_query, b_query, w_key, w_value, b_value, w_out, b_out, ln2_gain, ln2_bias, w_up, b_up, w_down, b_down, lnp_gain, lnp_bias, cross_wk, cross_wv, cross_bv):
    qk_scale = HEAD_DIM ** -0.25
    row_count = BATCH_SIZE * FRAMES
    residual = x.astype(jnp.float32).reshape(row_count, D_MODEL)
    normed = layer_norm(residual, ln1_gain, ln1_bias).astype(jnp.bfloat16)
    queries = ((jnp.dot(normed, w_query, preferred_element_type=jnp.float32) + b_query.astype(jnp.float32)) * qk_scale).astype(jnp.bfloat16)
    key_rows = (jnp.dot(normed, w_key, preferred_element_type=jnp.float32) * qk_scale).astype(jnp.bfloat16)
    value_rows = (jnp.dot(normed, w_value, preferred_element_type=jnp.float32) + b_value.astype(jnp.float32)).astype(jnp.bfloat16)

    def split_heads(rows_in):
        return rows_in.reshape(BATCH_SIZE, FRAMES, NUM_HEADS, HEAD_DIM).transpose(0, 2, 1, 3).reshape(BATCH_SIZE * NUM_HEADS, FRAMES, HEAD_DIM)

    def head_attention(operands):
        q_head, k_head, v_head = operands
        scores = jnp.dot(q_head, k_head.T, preferred_element_type=jnp.float32)
        attn_probs = jax.nn.softmax(scores, axis=-1).astype(jnp.bfloat16)
        return jnp.dot(attn_probs, v_head, preferred_element_type=jnp.float32).astype(jnp.bfloat16)

    attended = lax.map(head_attention, (split_heads(queries), split_heads(key_rows), split_heads(value_rows)))
    attended = attended.reshape(BATCH_SIZE, NUM_HEADS, FRAMES, HEAD_DIM).transpose(0, 2, 1, 3).reshape(row_count, D_MODEL)
    residual = residual + jnp.dot(attended, w_out, preferred_element_type=jnp.float32) + b_out.astype(jnp.float32)
    normed = layer_norm(residual, ln2_gain, ln2_bias).astype(jnp.bfloat16)
    hidden = jax.nn.gelu(jnp.dot(normed, w_up, preferred_element_type=jnp.float32) + b_up.astype(jnp.float32), approximate=False).astype(jnp.bfloat16)
    residual = residual + jnp.dot(hidden, w_down, preferred_element_type=jnp.float32) + b_down.astype(jnp.float32)
    y_rows = layer_norm(residual, lnp_gain, lnp_bias).astype(jnp.bfloat16)

    def layer_cache(layer_weights):
        wk_layer, wv_layer, bv_layer = layer_weights
        k_layer = jnp.dot(y_rows, wk_layer, preferred_element_type=jnp.float32).astype(jnp.bfloat16)
        v_layer = (jnp.dot(y_rows, wv_layer, preferred_element_type=jnp.float32) + bv_layer.astype(jnp.float32)).astype(jnp.bfloat16)
        return k_layer, v_layer

    k_all, v_all = lax.map(layer_cache, (cross_wk, cross_wv, cross_bv))
    cache_shape = (DEC_LAYERS, BATCH_SIZE, FRAMES, NUM_HEADS, HEAD_DIM)
    return k_all.reshape(cache_shape), v_all.reshape(cache_shape)
```

```python
import functools
import jax
import jax.numpy as jnp
from jax import lax
from jax.experimental import pallas as pl
from jax.experimental.pallas import tpu as pltpu
from jax.sharding import PartitionSpec as P

HEAD_DIM = 64
LN_EPS = 1e-5
SQRT_HALF = 0.5 ** 0.5
PAIR = 2 * HEAD_DIM
VMEM_BYTES = 63 * 1024 * 1024
CORES = 2
MESH_ID = pl.DeviceIdType.MESH
NT = (((1,), (1,)), ((), ()))


def norm_rows(rows, gain, bias):
    mean_val = jnp.mean(rows, axis=-1, keepdims=True)
    centered = rows - mean_val
    variance = jnp.mean(centered * centered, axis=-1, keepdims=True)
    return centered * lax.rsqrt(variance + LN_EPS) * gain + bias


def f32(ref):
    return ref[...].astype(jnp.float32)


def vec(ref):
    return f32(ref).reshape(1, ref.shape[0])


def encoder_kernel(x_hbm, wq_hbm, wk_hbm, wv_hbm, wo_hbm, wu_hbm, wd_hbm,
                   gain1_ref, bias1_ref, bq_ref, bv_ref, bo_ref, gain2_ref, bias2_ref, bu_ref, bd_ref, gainp_ref, biasp_ref,
                   y_all, a_all, x_buf, y_buf, wq_ref, wk_ref, wkt_ref, wv_ref, wo_ref, wu_ref, wd_ref, kt_ref, v_ref, att_ref,
                   load_sem, keep_sem, a_send, a_recv, y_send, y_recv):
    clips, frames, d_model = x_hbm.shape
    chips = y_all.shape[2]
    half = frames // 2
    me = lax.axis_index('sp')
    core, chip = lax.rem(me, CORES), lax.div(me, CORES)
    other = 1 - core
    rchip, lchip, far = lax.rem(chip + 1, chips), lax.rem(chip + chips - 1, chips), lax.rem(chip + 2, chips)
    right, left, partner = {'sp': rchip * CORES + core}, {'sp': lchip * CORES + core}, {'sp': chip * CORES + other}

    loads = [pltpu.make_async_copy(x_hbm.at[pl.ds(0, 2)], x_buf.at[pl.ds(0, 2)], load_sem.at[0]),
             pltpu.make_async_copy(x_hbm.at[pl.ds(2, clips - 2)], x_buf.at[pl.ds(2, clips - 2)], load_sem.at[1])]
    pairs = ((wq_hbm, wq_ref), (wk_hbm, wk_ref), (wv_hbm, wv_ref), (wo_hbm, wo_ref), (wu_hbm, wu_ref), (wd_hbm, wd_ref))
    loads += [pltpu.make_async_copy(src, dst, load_sem.at[2 + i]) for i, (src, dst) in enumerate(pairs)]
    for load in loads:
        load.start()

    barrier = pltpu.get_barrier_semaphore()
    for peer in (left, right, partner):
        pl.semaphore_signal(barrier, inc=1, device_id=peer, device_id_type=MESH_ID)
    pl.semaphore_wait(barrier, 3)

    def remote(src, dst, send, recv, peer):
        return pltpu.make_async_remote_copy(src_ref=src, dst_ref=dst, send_sem=send, recv_sem=recv, device_id=peer, device_id_type=MESH_ID)

    def ring(buf, send, recv, own):
        def shard(clip, where):
            return buf.at[clip, core, where]

        def lower(clip, where):
            return buf.at[clip, core, where, pl.ds(0, half)]

        def upper(clip, where):
            return buf.at[clip, core, where, pl.ds(half, half)]

        def out_right(clip):
            return remote(own(clip), shard(clip, chip), send.at[0, clip], recv.at[0, clip], right)

        def out_left(clip):
            return remote(own(clip), shard(clip, chip), send.at[1, clip], recv.at[1, clip], left)

        def fwd_right(clip):
            return remote(lower(clip, lchip), lower(clip, lchip), send.at[2, clip], recv.at[2, clip], right)

        def fwd_left(clip):
            return remote(upper(clip, rchip), upper(clip, rchip), send.at[3, clip], recv.at[3, clip], left)

        def across(clip):
            return remote(buf.at[clip, core], buf.at[clip, core], send.at[4, clip], recv.at[4, clip], partner)

        def first(clip):
            out_right(clip).start()
            out_left(clip).start()

        def relay(clip):
            remote(shard(clip, lchip), shard(clip, lchip), send.at[0, clip], recv.at[0, clip], right).wait_recv()
            fwd_right(clip).start()
            remote(shard(clip, rchip), shard(clip, rchip), send.at[1, clip], recv.at[1, clip], left).wait_recv()
            fwd_left(clip).start()

        def push(clip):
            remote(lower(clip, far), lower(clip, far), send.at[2, clip], recv.at[2, clip], right).wait_recv()
            remote(upper(clip, far), upper(clip, far), send.at[3, clip], recv.at[3, clip], left).wait_recv()
            across(clip).start()

        def finish(clip):
            remote(buf.at[clip, other], buf.at[clip, other], send.at[4, clip], recv.at[4, clip], partner).wait_recv()

        def sent(clip):
            for copy in (out_right(clip), out_left(clip), fwd_right(clip), fwd_left(clip), across(clip)):
                copy.wait_send()

        return first, relay, push, finish, sent

    a_first, a_relay, a_push, a_finish, a_sent = ring(a_all, a_send, a_recv, lambda clip: a_all.at[clip, core, chip])
    y_first, y_relay, y_push, y_finish, y_sent = ring(y_all, y_send, y_recv, lambda clip: y_buf.at[clip])

    def keep(clip):
        return pltpu.make_async_copy(y_buf.at[clip], y_all.at[clip, core, chip], keep_sem.at[clip])

    gain1, bias1 = vec(gain1_ref), vec(bias1_ref)

    def norm(clip):
        a_all[clip, core, chip] = norm_rows(x_buf[clip].astype(jnp.float32), gain1, bias1).astype(jnp.bfloat16)

    def norm_range(lo, hi):
        @pl.loop(lo, hi)
        def _(clip):
            norm(clip)

    loads[0].wait()
    norm(0)
    norm(1)
    a_first(0)
    a_first(1)
    loads[1].wait()
    third = (clips - 2) // 3
    norm_range(2, 2 + third)
    a_relay(0)
    a_first(2)
    norm_range(2 + third, 2 + 2 * third)
    a_relay(1)
    a_first(3)
    norm_range(2 + 2 * third, clips)
    for load in loads[2:]:
        load.wait()
    wkt_ref[...] = wk_ref[...].T
    a_push(0)

    qk_scale = HEAD_DIM ** -0.25
    low = lax.broadcasted_iota(jnp.int32, (frames, PAIR), 1) < HEAD_DIM

    def attention(clip):
        own = a_all[clip, core, chip]
        rows = a_all[clip].reshape(CORES * chips * frames, d_model)
        queries = ((jnp.dot(own, wq_ref[...], preferred_element_type=jnp.float32) + vec(bq_ref)) * qk_scale).astype(jnp.bfloat16)
        kt_ref[...] = (lax.dot_general(wkt_ref[...], rows, NT, preferred_element_type=jnp.float32) * qk_scale).astype(jnp.bfloat16)
        v_ref[...] = (jnp.dot(rows, wv_ref[...], preferred_element_type=jnp.float32) + vec(bv_ref)).astype(jnp.bfloat16)
        for pair in range(d_model // PAIR):
            cols = slice(pair * PAIR, (pair + 1) * PAIR)
            q_pair = queries[:, cols]
            kt_pair = kt_ref[cols, :]
            v_pair = v_ref[:, cols]
            parts = []
            for side in range(2):
                q_head = jnp.where(low if side == 0 else jnp.logical_not(low), q_pair, jnp.zeros_like(q_pair))
                scores = jnp.dot(q_head, kt_pair, preferred_element_type=jnp.float32)
                top = jnp.max(scores, axis=-1, keepdims=True)
                weights = jnp.exp(scores - top)
                total = jnp.sum(weights, axis=-1, keepdims=True)
                mixed = jnp.dot(weights.astype(jnp.bfloat16), v_pair, preferred_element_type=jnp.float32)
                parts.append(mixed / total)
            att_ref[:, cols] = jnp.where(low, parts[0], parts[1]).astype(jnp.bfloat16)

    def feed_forward(clip):
        residual = x_buf[clip].astype(jnp.float32)
        residual = residual + jnp.dot(att_ref[...], wo_ref[...], preferred_element_type=jnp.float32) + vec(bo_ref)
        normed = norm_rows(residual, vec(gain2_ref), vec(bias2_ref)).astype(jnp.bfloat16)
        acc = residual
        for start in range(0, wu_ref.shape[1], d_model):
            cols = slice(start, start + d_model)
            up = jnp.dot(normed, wu_ref[:, cols], preferred_element_type=jnp.float32) + bu_ref[cols].astype(jnp.float32).reshape(1, d_model)
            hidden = (0.5 * up * (1.0 + lax.erf(up * SQRT_HALF))).astype(jnp.bfloat16)
            acc = acc + jnp.dot(hidden, wd_ref[cols, :], preferred_element_type=jnp.float32)
        acc = acc + vec(bd_ref)
        y_buf[clip] = norm_rows(acc, vec(gainp_ref), vec(biasp_ref)).astype(jnp.bfloat16)

    @pl.loop(0, clips)
    def _(clip):
        @pl.when(clip + 2 < clips)
        def _():
            a_relay(clip + 2)

        @pl.when(clip + 4 < clips)
        def _():
            a_first(clip + 4)

        @pl.when(clip + 1 < clips)
        def _():
            a_push(clip + 1)

        a_finish(clip)
        attention(clip)

        @pl.when(clip >= 1)
        def _():
            y_relay(clip - 1)

        feed_forward(clip)
        keep(clip).start()
        y_first(clip)

        @pl.when(clip >= 2)
        def _():
            keep(clip - 2).wait()
            y_push(clip - 2)

    y_relay(clips - 1)
    keep(clips - 2).wait()
    y_push(clips - 2)
    keep(clips - 1).wait()
    y_push(clips - 1)

    @pl.loop(0, clips)
    def _(clip):
        y_finish(clip)
        a_sent(clip)
        y_sent(clip)


def cache_kernel(y_ref, wk_ref, wv_ref, bv_ref, k_ref, v_ref, bias_ref):
    @pl.when(pl.program_id(0) == 0)
    def _():
        layers, width = bv_ref.shape
        columns = f32(bv_ref).T
        for layer in range(layers):
            bias_ref[layer * width:(layer + 1) * width, :] = columns[:, layer:layer + 1]

    cores, chips = y_ref.shape[1:3]
    rows = jnp.concatenate([y_ref[0, core, chip] for chip in range(chips) for core in range(cores)], axis=0)
    shape = k_ref.shape
    keys = lax.dot_general(wk_ref[...], rows, NT, preferred_element_type=jnp.float32)
    k_ref[...] = keys.astype(jnp.bfloat16).reshape(shape)
    values = lax.dot_general(wv_ref[...], rows, NT, preferred_element_type=jnp.float32) + bias_ref[...]
    v_ref[...] = values.astype(jnp.bfloat16).reshape(shape)


def whole(*shape):
    return pl.BlockSpec(shape, lambda i: (0,) * len(shape))


def solution(mesh):
    def device_fn(x_rows, ln1_gain, ln1_bias, w_query, b_query, w_key, w_value, b_value, w_out, b_out, ln2_gain, ln2_bias, w_up, b_up, w_down, b_down, lnp_gain, lnp_bias, cross_wk, cross_wv, cross_bv):
        batch, frames_dev, d_model = x_rows.shape
        layers, _, width = cross_wk.shape
        devices = lax.axis_size('sp')
        chips = devices // CORES
        frames_all = frames_dev * devices
        wide = w_up.shape[1]
        bf16 = jnp.bfloat16
        hbm = pl.BlockSpec(memory_space=pl.ANY)
        vmem = pl.BlockSpec(memory_space=pltpu.VMEM)
        per_clip = pltpu.SemaphoreType.DMA((5, batch))
        y_all = pl.pallas_call(
            encoder_kernel,
            in_specs=[hbm] * 7 + [vmem] * 11,
            out_specs=hbm,
            out_shape=jax.ShapeDtypeStruct((batch, CORES, chips, frames_dev, d_model), bf16),
            scratch_shapes=[
                pltpu.VMEM((batch, CORES, chips, frames_dev, d_model), bf16),
                pltpu.VMEM((batch, frames_dev, d_model), bf16),
                pltpu.VMEM((batch, frames_dev, d_model), bf16),
                pltpu.VMEM((d_model, d_model), bf16), pltpu.VMEM((d_model, d_model), bf16), pltpu.VMEM((d_model, d_model), bf16),
                pltpu.VMEM((d_model, d_model), bf16), pltpu.VMEM((d_model, d_model), bf16),
                pltpu.VMEM((d_model, wide), bf16), pltpu.VMEM((wide, d_model), bf16),
                pltpu.VMEM((d_model, frames_all), bf16), pltpu.VMEM((frames_all, d_model), bf16),
                pltpu.VMEM((frames_dev, d_model), bf16),
                pltpu.SemaphoreType.DMA((8,)), pltpu.SemaphoreType.DMA((batch,)),
                per_clip, per_clip, per_clip, per_clip,
            ],
            compiler_params=pltpu.CompilerParams(collective_id=0, has_side_effects=True, vmem_limit_bytes=VMEM_BYTES),
            name="encoder",
        )(x_rows, w_query, w_key, w_value, w_out, w_up, w_down, ln1_gain, ln1_bias, b_query, b_value, b_out,
          ln2_gain, ln2_bias, b_up, b_down, lnp_gain, lnp_bias)

        ckt = jnp.swapaxes(cross_wk, 1, 2).reshape(layers * width, d_model)
        cvt = jnp.swapaxes(cross_wv, 1, 2).reshape(layers * width, d_model)
        shape = jax.ShapeDtypeStruct((layers, batch, width, frames_all), bf16)
        wspec = whole(layers * width, d_model)
        blk = pl.BlockSpec((layers, 1, width, frames_all), lambda i: (0, i, 0, 0))
        held = pl.pallas_call(
            cache_kernel, grid=(batch,),
            in_specs=[pl.BlockSpec((1, CORES, chips, frames_dev, d_model), lambda i: (i, 0, 0, 0, 0)), wspec, wspec, whole(layers, width)],
            out_specs=[blk, blk], out_shape=[shape, shape],
            scratch_shapes=[pltpu.VMEM((layers * width, 1), jnp.float32)],
            compiler_params=pltpu.CompilerParams(dimension_semantics=("arbitrary",), vmem_limit_bytes=VMEM_BYTES),
            name="caches",
        )(y_all, ckt, cvt, cross_bv)
        heads = width // HEAD_DIM
        return tuple(jnp.moveaxis(buf.reshape(layers, batch, heads, HEAD_DIM, frames_all), 4, 2) for buf in held)

    in_specs = (P('dp', 'sp', None),) + (P(),) * 17 + (P(None, None, 'sp'), P(None, None, 'sp'), P(None, 'sp'))
    out_specs = (P(None, 'dp', None, 'sp', None), P(None, 'dp', None, 'sp', None))
    return jax.shard_map(device_fn, mesh=mesh, in_specs=in_specs, out_specs=out_specs, check_vma=False)
```

```python
import functools
import jax
import jax.numpy as jnp
from jax import lax
from jax.experimental import pallas as pl
from jax.experimental.pallas import tpu as pltpu
from jax.sharding import PartitionSpec as P

HEAD_DIM = 64
LN_EPS = 1e-5
SQRT_HALF = 0.5 ** 0.5
PAIR = 2 * HEAD_DIM
VMEM_BYTES = 63 * 1024 * 1024
CORES = 2
KINDS = 13
RELAY_LAG = 2
PUSH_LAG = 4
MESH_ID = pl.DeviceIdType.MESH
NT = (((1,), (1,)), ((), ()))


def norm_rows(rows, gain, bias):
    mean_val = jnp.mean(rows, axis=-1, keepdims=True)
    centered = rows - mean_val
    variance = jnp.mean(centered * centered, axis=-1, keepdims=True)
    return centered * lax.rsqrt(variance + LN_EPS) * gain + bias


def f32(ref):
    return ref[...].astype(jnp.float32)


def vec(ref):
    return f32(ref).reshape(1, ref.shape[0])


def encoder_kernel(x_hbm, wq_hbm, wk_hbm, wv_hbm, wo_hbm, wu_hbm, wd_hbm,
                   gain1_ref, bias1_ref, bq_ref, bv_ref, bo_ref, gain2_ref, bias2_ref, bu_ref, bd_ref, gainp_ref, biasp_ref,
                   y_all, x_buf, relay_buf, y_buf, wq_ref, wk_ref, wkt_ref, wv_ref, wo_ref, wu_ref, wd_ref, a_ref, q_ref, kt_ref, v_ref, att_ref,
                   load_sem, keep_sem, x_send, x_recv, y_send, y_recv):
    chips, _, per, blocks, frames, d_model = y_all.shape
    half = frames // 2
    items = per * blocks
    me = lax.axis_index('sp')
    core, chip = lax.rem(me, CORES), lax.div(me, CORES)
    other = 1 - core
    rchip, lchip, far = lax.rem(chip + 1, chips), lax.rem(chip + chips - 1, chips), lax.rem(chip + 2, chips)
    right, left, partner = {'sp': rchip * CORES + core}, {'sp': lchip * CORES + core}, {'sp': chip * CORES + other}

    mine = [pltpu.make_async_copy(x_hbm.at[me * per + c], x_buf.at[c, me], load_sem.at[c]) for c in range(per)]
    pairs = ((wq_hbm, wq_ref), (wk_hbm, wk_ref), (wv_hbm, wv_ref), (wo_hbm, wo_ref), (wu_hbm, wu_ref), (wd_hbm, wd_ref))
    loads = [pltpu.make_async_copy(src, dst, load_sem.at[per + i]) for i, (src, dst) in enumerate(pairs)]

    around = [where * CORES + k for where in (rchip, lchip) for k in range(CORES)] + [chip * CORES + other]
    barrier = pltpu.get_barrier_semaphore()
    for peer in around:
        pl.semaphore_signal(barrier, inc=1, device_id={'sp': peer}, device_id_type=MESH_ID)
    pl.semaphore_wait(barrier, len(around))

    def remote(src, dst, send, recv, peer):
        return pltpu.make_async_remote_copy(src_ref=src, dst_ref=dst, send_sem=send, recv_sem=recv, device_id=peer, device_id_type=MESH_ID)

    rows_lo, rows_hi = pl.ds(0, half), pl.ds(half, half)

    def scatter(c):
        def link(kind, src, dst, mark, peer):
            return remote(src, dst, x_send.at[c, kind], x_recv.at[c, mark], {'sp': peer})

        copies = []
        for k in range(CORES):
            away = x_hbm.at[(far * CORES + k) * per + c]
            copies.append(link(5 + k, away.at[rows_lo], relay_buf.at[0, c, k], 5 + k, rchip * CORES + core))
            copies.append(link(7 + k, away.at[rows_hi], relay_buf.at[1, c, k], 7 + k, lchip * CORES + core))
        for k in range(CORES):
            copies.append(link(1 + k, x_hbm.at[(rchip * CORES + k) * per + c], x_buf.at[c, me], 1 + core, rchip * CORES + k))
            copies.append(link(3 + k, x_hbm.at[(lchip * CORES + k) * per + c], x_buf.at[c, me], 3 + core, lchip * CORES + k))
        copies.append(link(0, x_hbm.at[(chip * CORES + other) * per + c], x_buf.at[c, me], 0, chip * CORES + other))
        return copies

    def onward(c):
        pairs = []
        for k in range(CORES):
            to_right = x_buf.at[c, lchip * CORES + core, rows_lo]
            to_left = x_buf.at[c, rchip * CORES + core, rows_hi]
            came_left, came_right = relay_buf.at[0, c, k], relay_buf.at[1, c, k]
            pairs.append((lambda ref=came_left, mark=5 + k: remote(ref, ref, x_send.at[c, mark], x_recv.at[c, mark], right).wait_recv(),
                          remote(came_left, to_right, x_send.at[c, 9 + k], x_recv.at[c, 9 + core], {'sp': rchip * CORES + k})))
            pairs.append((lambda ref=came_right, mark=7 + k: remote(ref, ref, x_send.at[c, mark], x_recv.at[c, mark], right).wait_recv(),
                          remote(came_right, to_left, x_send.at[c, 11 + k], x_recv.at[c, 11 + core], {'sp': lchip * CORES + k})))
        return pairs

    def send_clip(c):
        for copy in scatter(c):
            copy.start()

    def relay_clip(c):
        for came, goes in onward(c):
            came()
            goes.start()

    def arrivals(c):
        def landed(mark, ref):
            return remote(ref, ref, x_send.at[c, mark], x_recv.at[c, mark], right)

        near = [(0, chip * CORES + other)]
        near += [(1 + k, lchip * CORES + k) for k in range(CORES)] + [(3 + k, rchip * CORES + k) for k in range(CORES)]
        groups = [(block, [landed(mark, x_buf.at[c, block])]) for mark, block in near]
        for k in range(CORES):
            block = far * CORES + k
            groups.append((block, [landed(9 + k, x_buf.at[c, block, rows_lo]), landed(11 + k, x_buf.at[c, block, rows_hi])]))
        return groups

    send_clip(0)
    for copy in mine:
        copy.start()
    for load in loads:
        load.start()

    def place(t, where):
        return y_all.at[where, core, lax.div(t, blocks), lax.rem(t, blocks)]

    def lower(t, where):
        return y_all.at[where, core, lax.div(t, blocks), lax.rem(t, blocks), pl.ds(0, half)]

    def upper(t, where):
        return y_all.at[where, core, lax.div(t, blocks), lax.rem(t, blocks), pl.ds(half, half)]

    def column(t, side):
        return y_all.at[pl.ds(0, chips), side, lax.div(t, blocks), lax.rem(t, blocks)]

    def out_right(t):
        return remote(y_buf.at[t], place(t, chip), y_send.at[0, t], y_recv.at[0, t], right)

    def out_left(t):
        return remote(y_buf.at[t], place(t, chip), y_send.at[1, t], y_recv.at[1, t], left)

    def fwd_right(t):
        return remote(lower(t, lchip), lower(t, lchip), y_send.at[2, t], y_recv.at[2, t], right)

    def fwd_left(t):
        return remote(upper(t, rchip), upper(t, rchip), y_send.at[3, t], y_recv.at[3, t], left)

    def across(t):
        return remote(column(t, core), column(t, core), y_send.at[4, t], y_recv.at[4, t], partner)

    def keep(t):
        return pltpu.make_async_copy(y_buf.at[t], place(t, chip), keep_sem.at[t])

    def first(t):
        keep(t).start()
        out_right(t).start()
        out_left(t).start()

    def relay(t):
        remote(place(t, lchip), place(t, lchip), y_send.at[0, t], y_recv.at[0, t], right).wait_recv()
        fwd_right(t).start()
        remote(place(t, rchip), place(t, rchip), y_send.at[1, t], y_recv.at[1, t], left).wait_recv()
        fwd_left(t).start()

    def push(t):
        keep(t).wait()
        remote(lower(t, far), lower(t, far), y_send.at[2, t], y_recv.at[2, t], right).wait_recv()
        remote(upper(t, far), upper(t, far), y_send.at[3, t], y_recv.at[3, t], left).wait_recv()
        across(t).start()

    qk_scale = HEAD_DIM ** -0.25
    low = lax.broadcasted_iota(jnp.int32, (half, PAIR), 1) < HEAD_DIM
    gain1, bias1 = vec(gain1_ref), vec(bias1_ref)

    def norm(c, block):
        a_ref[block] = norm_rows(x_buf[c, block].astype(jnp.float32), gain1, bias1).astype(jnp.bfloat16)

    def project():
        rows = a_ref[...].reshape(blocks * frames, d_model)
        queries = ((jnp.dot(rows, wq_ref[...], preferred_element_type=jnp.float32) + vec(bq_ref)) * qk_scale).astype(jnp.bfloat16)
        q_ref[...] = queries.reshape(blocks, frames, d_model)
        kt_ref[...] = (lax.dot_general(wkt_ref[...], rows, NT, preferred_element_type=jnp.float32) * qk_scale).astype(jnp.bfloat16)
        v_ref[...] = (jnp.dot(rows, wv_ref[...], preferred_element_type=jnp.float32) + vec(bv_ref)).astype(jnp.bfloat16)

    def attention(block):
        tasks = [(pair, piece, side) for pair in range(d_model // PAIR) for piece in range(2) for side in range(2)]
        held = {}

        def score(task):
            pair, piece, side = task
            cols = slice(pair * PAIR, (pair + 1) * PAIR)
            q_pair = q_ref[block, piece * half:(piece + 1) * half, cols]
            q_head = jnp.where(low if side == 0 else jnp.logical_not(low), q_pair, jnp.zeros_like(q_pair))
            return jnp.dot(q_head, kt_ref[cols, :], preferred_element_type=jnp.float32)

        def soften(scores):
            top = jnp.max(scores, axis=-1, keepdims=True)
            weights = jnp.exp(scores - top)
            return weights.astype(jnp.bfloat16), jnp.sum(weights, axis=-1, keepdims=True)

        def mix(task, weights, total):
            pair, piece, side = task
            cols = slice(pair * PAIR, (pair + 1) * PAIR)
            out = jnp.dot(weights, v_ref[:, cols], preferred_element_type=jnp.float32) / total
            if side == 0:
                held[0] = out
            else:
                att_ref[piece * half:(piece + 1) * half, cols] = jnp.where(low, held[0], out).astype(jnp.bfloat16)

        scores, waiting = score(tasks[0]), None
        for i, task in enumerate(tasks):
            following = score(tasks[i + 1]) if i + 1 < len(tasks) else None
            weights, total = soften(scores)
            if waiting is not None:
                mix(*waiting)
            waiting, scores = (task, weights, total), following
        mix(*waiting)

    def feed_forward(c, block, t):
        residual = x_buf[c, block].astype(jnp.float32)
        residual = residual + jnp.dot(att_ref[...], wo_ref[...], preferred_element_type=jnp.float32) + vec(bo_ref)
        normed = norm_rows(residual, vec(gain2_ref), vec(bias2_ref)).astype(jnp.bfloat16)
        hidden = []
        for start in range(0, wu_ref.shape[1], d_model):
            cols = slice(start, start + d_model)
            up = jnp.dot(normed, wu_ref[:, cols], preferred_element_type=jnp.float32) + bu_ref[cols].astype(jnp.float32).reshape(1, d_model)
            halved = 0.5 * up
            hidden.append((halved + halved * lax.erf(up * SQRT_HALF)).astype(jnp.bfloat16))
        acc = residual + jnp.dot(jnp.concatenate(hidden, axis=1), wd_ref[...], preferred_element_type=jnp.float32) + vec(bd_ref)
        y_buf[t] = norm_rows(acc, vec(gainp_ref), vec(biasp_ref)).astype(jnp.bfloat16)

    relay_clip(0)
    if per > 1:
        send_clip(1)
    for load in loads:
        load.wait()
    wkt_ref[...] = wk_ref[...].T

    @pl.loop(0, per)
    def _(c):
        pltpu.make_async_copy(x_hbm.at[me * per + c], x_buf.at[c, me], load_sem.at[c]).wait()
        norm(c, me)
        for block, copies in arrivals(c):
            for copy in copies:
                copy.wait_recv()
            norm(c, block)
        project()

        @pl.when(c + 1 < per)
        def _():
            relay_clip(c + 1)

        @pl.when(c + 2 < per)
        def _():
            send_clip(c + 2)

        @pl.loop(0, blocks)
        def _(block):
            t = c * blocks + block
            attention(block)

            @pl.when(t >= RELAY_LAG)
            def _():
                relay(t - RELAY_LAG)

            feed_forward(c, block, t)
            first(t)

            @pl.when(t >= PUSH_LAG)
            def _():
                push(t - PUSH_LAG)

    for back in range(PUSH_LAG, 0, -1):
        if back <= RELAY_LAG:
            relay(items - back)
    for back in range(PUSH_LAG, 0, -1):
        push(items - back)

    @pl.loop(0, items)
    def _(t):
        remote(column(t, other), column(t, other), y_send.at[4, t], y_recv.at[4, t], partner).wait_recv()
        for copy in (out_right(t), out_left(t), fwd_right(t), fwd_left(t), across(t)):
            copy.wait_send()

    @pl.loop(0, per)
    def _(c):
        for copy in scatter(c):
            copy.wait_send()
        for _, goes in onward(c):
            goes.wait_send()


def cache_kernel(y_ref, wk_ref, wv_ref, bv_ref, k_ref, v_ref, bias_ref):
    @pl.when(pl.program_id(0) == 0)
    def _():
        layers, width = bv_ref.shape
        columns = f32(bv_ref).T
        for layer in range(layers):
            bias_ref[layer * width:(layer + 1) * width, :] = columns[:, layer:layer + 1]

    rows = y_ref[0]
    shape = k_ref.shape
    keys = lax.dot_general(wk_ref[...], rows, NT, preferred_element_type=jnp.float32)
    k_ref[...] = keys.astype(jnp.bfloat16).reshape(shape)
    values = lax.dot_general(wv_ref[...], rows, NT, preferred_element_type=jnp.float32) + bias_ref[...]
    v_ref[...] = values.astype(jnp.bfloat16).reshape(shape)


def whole(*shape):
    return pl.BlockSpec(shape, lambda i: (0,) * len(shape))


def solution(mesh):
    def device_fn(x_rows, ln1_gain, ln1_bias, w_query, b_query, w_key, w_value, b_value, w_out, b_out, ln2_gain, ln2_bias, w_up, b_up, w_down, b_down, lnp_gain, lnp_bias, cross_wk, cross_wv, cross_bv):
        batch, frames_dev, d_model = x_rows.shape
        layers, _, width = cross_wk.shape
        devices = lax.axis_size('sp')
        chips = devices // CORES
        frames_all = frames_dev * devices
        wide = w_up.shape[1]
        bf16 = jnp.bfloat16
        hbm = pl.BlockSpec(memory_space=pl.ANY)
        vmem = pl.BlockSpec(memory_space=pltpu.VMEM)
        per = batch // devices
        clip_rows = pltpu.VMEM((devices, frames_dev, d_model), bf16)
        square = pltpu.VMEM((d_model, d_model), bf16)
        y_all = pl.pallas_call(
            encoder_kernel,
            in_specs=[hbm] * 7 + [vmem] * 11,
            out_specs=hbm,
            out_shape=jax.ShapeDtypeStruct((chips, CORES, per, devices, frames_dev, d_model), bf16),
            scratch_shapes=[
                pltpu.VMEM((per, devices, frames_dev, d_model), bf16),
                pltpu.VMEM((2, per, CORES, frames_dev // 2, d_model), bf16),
                pltpu.VMEM((batch, frames_dev, d_model), bf16),
                square, square, square, square, square,
                pltpu.VMEM((d_model, wide), bf16), pltpu.VMEM((wide, d_model), bf16),
                clip_rows, clip_rows,
                pltpu.VMEM((d_model, frames_all), bf16), pltpu.VMEM((frames_all, d_model), bf16),
                pltpu.VMEM((frames_dev, d_model), bf16),
                pltpu.SemaphoreType.DMA((per + 6,)), pltpu.SemaphoreType.DMA((batch,)),
                pltpu.SemaphoreType.DMA((per, KINDS)), pltpu.SemaphoreType.DMA((per, KINDS)),
                pltpu.SemaphoreType.DMA((5, batch)), pltpu.SemaphoreType.DMA((5, batch)),
            ],
            compiler_params=pltpu.CompilerParams(collective_id=0, has_side_effects=True, vmem_limit_bytes=VMEM_BYTES),
            name="encoder",
        )(x_rows, w_query, w_key, w_value, w_out, w_up, w_down, ln1_gain, ln1_bias, b_query, b_value, b_out,
          ln2_gain, ln2_bias, b_up, b_down, lnp_gain, lnp_bias)
        y_all = y_all.reshape(batch, frames_all, d_model)

        ckt = jnp.swapaxes(cross_wk, 1, 2).reshape(layers * width, d_model)
        cvt = jnp.swapaxes(cross_wv, 1, 2).reshape(layers * width, d_model)
        shape = jax.ShapeDtypeStruct((layers, batch, width, frames_all), bf16)
        wspec = whole(layers * width, d_model)
        blk = pl.BlockSpec((layers, 1, width, frames_all), lambda i: (0, i, 0, 0))
        held = pl.pallas_call(
            cache_kernel, grid=(batch,),
            in_specs=[pl.BlockSpec((1, frames_all, d_model), lambda i: (i, 0, 0)), wspec, wspec, whole(layers, width)],
            out_specs=[blk, blk], out_shape=[shape, shape],
            scratch_shapes=[pltpu.VMEM((layers * width, 1), jnp.float32)],
            compiler_params=pltpu.CompilerParams(dimension_semantics=("arbitrary",), vmem_limit_bytes=VMEM_BYTES),
            name="caches",
        )(y_all, ckt, cvt, cross_bv)
        heads = width // HEAD_DIM
        return tuple(jnp.moveaxis(buf.reshape(layers, batch, heads, HEAD_DIM, frames_all), 4, 2) for buf in held)

    in_specs = (P('dp', 'sp', None),) + (P(),) * 17 + (P(None, None, 'sp'), P(None, None, 'sp'), P(None, 'sp'))
    out_specs = (P(None, 'dp', None, 'sp', None), P(None, 'dp', None, 'sp', None))
    return jax.shard_map(device_fn, mesh=mesh, in_specs=in_specs, out_specs=out_specs, check_vma=False)
```

```python
import functools
import jax
import jax.numpy as jnp
from jax import lax
from jax.experimental import pallas as pl
from jax.experimental.pallas import tpu as pltpu
from jax.sharding import PartitionSpec as P

HEAD_DIM = 64
LN_EPS = 1e-5
SQRT_HALF = 0.5 ** 0.5
PAIR = 2 * HEAD_DIM
VMEM_BYTES = 63 * 1024 * 1024
CORES = 2
KINDS = 13
RELAY_LAG = 2
PUSH_LAG = 4
MESH_ID = pl.DeviceIdType.MESH
NT = (((1,), (1,)), ((), ()))


def norm_rows(rows, gain, bias):
    mean_val = jnp.mean(rows, axis=-1, keepdims=True)
    centered = rows - mean_val
    variance = jnp.mean(centered * centered, axis=-1, keepdims=True)
    return centered * lax.rsqrt(variance + LN_EPS) * gain + bias


def f32(ref):
    return ref[...].astype(jnp.float32)


def vec(ref):
    return f32(ref).reshape(1, ref.shape[0])


def encoder_kernel(x_hbm, wq_hbm, wk_hbm, wv_hbm, wo_hbm, wu_hbm, wd_hbm,
                   gain1_ref, bias1_ref, bq_ref, bv_ref, bo_ref, gain2_ref, bias2_ref, bu_ref, bd_ref, gainp_ref, biasp_ref,
                   y_all, x_buf, relay_buf, y_buf, wq_ref, wk_ref, wkt_ref, wv_ref, wo_ref, wu_ref, wd_ref, a_ref, q_ref, kt_ref, v_ref, att_ref,
                   load_sem, keep_sem, x_send, x_recv, y_send, y_recv):
    chips, _, per, blocks, frames, d_model = y_all.shape
    half = frames // 2
    items = per * blocks
    me = lax.axis_index('sp')
    core, chip = lax.rem(me, CORES), lax.div(me, CORES)
    other = 1 - core
    rchip, lchip, far = lax.rem(chip + 1, chips), lax.rem(chip + chips - 1, chips), lax.rem(chip + 2, chips)
    right, left, partner = {'sp': rchip * CORES + core}, {'sp': lchip * CORES + core}, {'sp': chip * CORES + other}

    mine = [pltpu.make_async_copy(x_hbm.at[me * per + c], x_buf.at[c, me], load_sem.at[c]) for c in range(per)]
    pairs = ((wq_hbm, wq_ref), (wk_hbm, wk_ref), (wv_hbm, wv_ref), (wo_hbm, wo_ref), (wu_hbm, wu_ref), (wd_hbm, wd_ref))
    loads = [pltpu.make_async_copy(src, dst, load_sem.at[per + i]) for i, (src, dst) in enumerate(pairs)]

    around = [where * CORES + k for where in (rchip, lchip) for k in range(CORES)] + [chip * CORES + other]
    barrier = pltpu.get_barrier_semaphore()
    for peer in around:
        pl.semaphore_signal(barrier, inc=1, device_id={'sp': peer}, device_id_type=MESH_ID)
    pl.semaphore_wait(barrier, len(around))

    def remote(src, dst, send, recv, peer):
        return pltpu.make_async_remote_copy(src_ref=src, dst_ref=dst, send_sem=send, recv_sem=recv, device_id=peer, device_id_type=MESH_ID)

    rows_lo, rows_hi = pl.ds(0, half), pl.ds(half, half)

    def scatter(c):
        def link(kind, src, dst, mark, peer):
            return remote(src, dst, x_send.at[c, kind], x_recv.at[c, mark], {'sp': peer})

        copies = []
        for k in range(CORES):
            away = x_hbm.at[(far * CORES + k) * per + c]
            copies.append(link(5 + k, away.at[rows_lo], relay_buf.at[0, c, k], 5 + k, rchip * CORES + core))
            copies.append(link(7 + k, away.at[rows_hi], relay_buf.at[1, c, k], 7 + k, lchip * CORES + core))
        for k in range(CORES):
            copies.append(link(1 + k, x_hbm.at[(rchip * CORES + k) * per + c], x_buf.at[c, me], 1 + core, rchip * CORES + k))
            copies.append(link(3 + k, x_hbm.at[(lchip * CORES + k) * per + c], x_buf.at[c, me], 3 + core, lchip * CORES + k))
        copies.append(link(0, x_hbm.at[(chip * CORES + other) * per + c], x_buf.at[c, me], 0, chip * CORES + other))
        return copies

    def onward(c):
        pairs = []
        for k in range(CORES):
            to_right = x_buf.at[c, lchip * CORES + core, rows_lo]
            to_left = x_buf.at[c, rchip * CORES + core, rows_hi]
            came_left, came_right = relay_buf.at[0, c, k], relay_buf.at[1, c, k]
            pairs.append((lambda ref=came_left, mark=5 + k: remote(ref, ref, x_send.at[c, mark], x_recv.at[c, mark], right).wait_recv(),
                          remote(came_left, to_right, x_send.at[c, 9 + k], x_recv.at[c, 9 + core], {'sp': rchip * CORES + k})))
            pairs.append((lambda ref=came_right, mark=7 + k: remote(ref, ref, x_send.at[c, mark], x_recv.at[c, mark], right).wait_recv(),
                          remote(came_right, to_left, x_send.at[c, 11 + k], x_recv.at[c, 11 + core], {'sp': lchip * CORES + k})))
        return pairs

    def send_clip(c):
        for copy in scatter(c):
            copy.start()

    def relay_clip(c):
        for came, goes in onward(c):
            came()
            goes.start()

    def arrivals(c):
        def landed(mark, ref):
            return remote(ref, ref, x_send.at[c, mark], x_recv.at[c, mark], right)

        near = [(0, chip * CORES + other)]
        near += [(1 + k, lchip * CORES + k) for k in range(CORES)] + [(3 + k, rchip * CORES + k) for k in range(CORES)]
        groups = [(block, [landed(mark, x_buf.at[c, block])]) for mark, block in near]
        for k in range(CORES):
            block = far * CORES + k
            groups.append((block, [landed(9 + k, x_buf.at[c, block, rows_lo]), landed(11 + k, x_buf.at[c, block, rows_hi])]))
        return groups

    send_clip(0)
    for copy in mine:
        copy.start()
    for load in loads:
        load.start()

    def place(t, where):
        return y_all.at[where, core, lax.div(t, blocks), lax.rem(t, blocks)]

    def lower(t, where):
        return y_all.at[where, core, lax.div(t, blocks), lax.rem(t, blocks), pl.ds(0, half)]

    def upper(t, where):
        return y_all.at[where, core, lax.div(t, blocks), lax.rem(t, blocks), pl.ds(half, half)]

    def column(t, side):
        return y_all.at[pl.ds(0, chips), side, lax.div(t, blocks), lax.rem(t, blocks)]

    def out_right(t):
        return remote(y_buf.at[t], place(t, chip), y_send.at[0, t], y_recv.at[0, t], right)

    def out_left(t):
        return remote(y_buf.at[t], place(t, chip), y_send.at[1, t], y_recv.at[1, t], left)

    def fwd_right(t):
        return remote(lower(t, lchip), lower(t, lchip), y_send.at[2, t], y_recv.at[2, t], right)

    def fwd_left(t):
        return remote(upper(t, rchip), upper(t, rchip), y_send.at[3, t], y_recv.at[3, t], left)

    def across(t):
        return remote(column(t, core), column(t, core), y_send.at[4, t], y_recv.at[4, t], partner)

    def keep(t):
        return pltpu.make_async_copy(y_buf.at[t], place(t, chip), keep_sem.at[t])

    def first(t):
        keep(t).start()
        out_right(t).start()
        out_left(t).start()

    def relay(t):
        remote(place(t, lchip), place(t, lchip), y_send.at[0, t], y_recv.at[0, t], right).wait_recv()
        fwd_right(t).start()
        remote(place(t, rchip), place(t, rchip), y_send.at[1, t], y_recv.at[1, t], left).wait_recv()
        fwd_left(t).start()

    def push(t):
        keep(t).wait()
        remote(lower(t, far), lower(t, far), y_send.at[2, t], y_recv.at[2, t], right).wait_recv()
        remote(upper(t, far), upper(t, far), y_send.at[3, t], y_recv.at[3, t], left).wait_recv()
        across(t).start()

    qk_scale = HEAD_DIM ** -0.25
    low = lax.broadcasted_iota(jnp.int32, (half, PAIR), 1) < HEAD_DIM
    gain1, bias1 = vec(gain1_ref), vec(bias1_ref)

    def norm(c, block):
        a_ref[block] = norm_rows(x_buf[c, block].astype(jnp.float32), gain1, bias1).astype(jnp.bfloat16)

    def project():
        rows = a_ref[...].reshape(blocks * frames, d_model)
        queries = ((jnp.dot(rows, wq_ref[...], preferred_element_type=jnp.float32) + vec(bq_ref)) * qk_scale).astype(jnp.bfloat16)
        q_ref[...] = queries.reshape(blocks, frames, d_model)
        kt_ref[...] = (lax.dot_general(wkt_ref[...], rows, NT, preferred_element_type=jnp.float32) * qk_scale).astype(jnp.bfloat16)
        v_ref[...] = (jnp.dot(rows, wv_ref[...], preferred_element_type=jnp.float32) + vec(bv_ref)).astype(jnp.bfloat16)

    def attention(block):
        tasks = [(pair, piece, side) for pair in range(d_model // PAIR) for piece in range(2) for side in range(2)]
        held = {}

        def score(task):
            pair, piece, side = task
            cols = slice(pair * PAIR, (pair + 1) * PAIR)
            q_pair = q_ref[block, piece * half:(piece + 1) * half, cols]
            q_head = jnp.where(low if side == 0 else jnp.logical_not(low), q_pair, jnp.zeros_like(q_pair))
            return jnp.dot(q_head, kt_ref[cols, :], preferred_element_type=jnp.float32)

        def soften(scores):
            top = jnp.max(scores, axis=-1, keepdims=True)
            weights = jnp.exp(scores - top)
            return weights.astype(jnp.bfloat16), jnp.sum(weights, axis=-1, keepdims=True)

        def mix(task, weights, total):
            pair, piece, side = task
            cols = slice(pair * PAIR, (pair + 1) * PAIR)
            out = jnp.dot(weights, v_ref[:, cols], preferred_element_type=jnp.float32) / total
            if side == 0:
                held[0] = out
            else:
                att_ref[piece * half:(piece + 1) * half, cols] = jnp.where(low, held[0], out).astype(jnp.bfloat16)

        scores, waiting = score(tasks[0]), None
        for i, task in enumerate(tasks):
            following = score(tasks[i + 1]) if i + 1 < len(tasks) else None
            weights, total = soften(scores)
            if waiting is not None:
                mix(*waiting)
            waiting, scores = (task, weights, total), following
        mix(*waiting)

    def feed_forward(c, block, t):
        residual = x_buf[c, block].astype(jnp.float32)
        residual = residual + jnp.dot(att_ref[...], wo_ref[...], preferred_element_type=jnp.float32) + vec(bo_ref)
        normed = norm_rows(residual, vec(gain2_ref), vec(bias2_ref)).astype(jnp.bfloat16)
        hidden = []
        for start in range(0, wu_ref.shape[1], d_model):
            cols = slice(start, start + d_model)
            up = jnp.dot(normed, wu_ref[:, cols], preferred_element_type=jnp.float32) + bu_ref[cols].astype(jnp.float32).reshape(1, d_model)
            halved = 0.5 * up
            hidden.append((halved + halved * lax.erf(up * SQRT_HALF)).astype(jnp.bfloat16))
        acc = residual + jnp.dot(jnp.concatenate(hidden, axis=1), wd_ref[...], preferred_element_type=jnp.float32) + vec(bd_ref)
        y_buf[t] = norm_rows(acc, vec(gainp_ref), vec(biasp_ref)).astype(jnp.bfloat16)

    relay_clip(0)
    if per > 1:
        send_clip(1)
    for load in loads:
        load.wait()
    wkt_ref[...] = wk_ref[...].T

    @pl.loop(0, per)
    def _(c):
        pltpu.make_async_copy(x_hbm.at[me * per + c], x_buf.at[c, me], load_sem.at[c]).wait()
        norm(c, me)
        for block, copies in arrivals(c):
            for copy in copies:
                copy.wait_recv()
            norm(c, block)
        project()

        @pl.when(c + 1 < per)
        def _():
            relay_clip(c + 1)

        @pl.when(c + 2 < per)
        def _():
            send_clip(c + 2)

        @pl.loop(0, blocks)
        def _(block):
            t = c * blocks + block
            attention(block)

            @pl.when(t >= RELAY_LAG)
            def _():
                relay(t - RELAY_LAG)

            feed_forward(c, block, t)
            first(t)

            @pl.when(t >= PUSH_LAG)
            def _():
                push(t - PUSH_LAG)

    for back in range(PUSH_LAG, 0, -1):
        if back <= RELAY_LAG:
            relay(items - back)
    for back in range(PUSH_LAG, 0, -1):
        push(items - back)

    @pl.loop(0, items)
    def _(t):
        remote(column(t, other), column(t, other), y_send.at[4, t], y_recv.at[4, t], partner).wait_recv()
        for copy in (out_right(t), out_left(t), fwd_right(t), fwd_left(t), across(t)):
            copy.wait_send()

    @pl.loop(0, per)
    def _(c):
        for copy in scatter(c):
            copy.wait_send()
        for _, goes in onward(c):
            goes.wait_send()


def cache_kernel(y_hbm, wk_ref, wv_ref, bv_ref, k_hbm, v_hbm, bias_ref, y_buf, k_buf, v_buf, in_sem, k_sem, v_sem):
    clips, depth = y_hbm.shape[0], y_buf.shape[0]
    layers, width = bv_ref.shape
    held = k_buf.shape[1:]

    def load(clip):
        slot = lax.rem(clip, depth)
        return pltpu.make_async_copy(y_hbm.at[clip], y_buf.at[slot], in_sem.at[slot])

    def store(buf, out, sem, clip):
        slot = lax.rem(clip, 2)
        return pltpu.make_async_copy(buf.at[slot], out.at[pl.ds(0, layers), clip], sem.at[slot])

    for clip in range(depth - 1):
        load(clip).start()
    columns = f32(bv_ref).T
    for layer in range(layers):
        bias_ref[layer * width:(layer + 1) * width, :] = columns[:, layer:layer + 1]

    @pl.loop(0, clips)
    def _(clip):
        load(clip).wait()

        @pl.when(clip + depth - 1 < clips)
        def _():
            load(clip + depth - 1).start()

        @pl.when(clip >= 2)
        def _():
            store(k_buf, k_hbm, k_sem, clip - 2).wait()
            store(v_buf, v_hbm, v_sem, clip - 2).wait()

        slot = lax.rem(clip, 2)
        rows = y_buf[lax.rem(clip, depth)]
        keys = lax.dot_general(wk_ref[...], rows, NT, preferred_element_type=jnp.float32)
        k_buf[slot] = keys.astype(jnp.bfloat16).reshape(held)
        store(k_buf, k_hbm, k_sem, clip).start()
        values = lax.dot_general(wv_ref[...], rows, NT, preferred_element_type=jnp.float32) + bias_ref[...]
        v_buf[slot] = values.astype(jnp.bfloat16).reshape(held)
        store(v_buf, v_hbm, v_sem, clip).start()

    for clip in range(clips - 2, clips):
        store(k_buf, k_hbm, k_sem, clip).wait()
        store(v_buf, v_hbm, v_sem, clip).wait()


def solution(mesh):
    def device_fn(x_rows, ln1_gain, ln1_bias, w_query, b_query, w_key, w_value, b_value, w_out, b_out, ln2_gain, ln2_bias, w_up, b_up, w_down, b_down, lnp_gain, lnp_bias, cross_wk, cross_wv, cross_bv):
        batch, frames_dev, d_model = x_rows.shape
        layers, _, width = cross_wk.shape
        devices = lax.axis_size('sp')
        chips = devices // CORES
        frames_all = frames_dev * devices
        wide = w_up.shape[1]
        bf16 = jnp.bfloat16
        hbm = pl.BlockSpec(memory_space=pl.ANY)
        vmem = pl.BlockSpec(memory_space=pltpu.VMEM)
        per = batch // devices
        clip_rows = pltpu.VMEM((devices, frames_dev, d_model), bf16)
        square = pltpu.VMEM((d_model, d_model), bf16)
        y_all = pl.pallas_call(
            encoder_kernel,
            in_specs=[hbm] * 7 + [vmem] * 11,
            out_specs=hbm,
            out_shape=jax.ShapeDtypeStruct((chips, CORES, per, devices, frames_dev, d_model), bf16),
            scratch_shapes=[
                pltpu.VMEM((per, devices, frames_dev, d_model), bf16),
                pltpu.VMEM((2, per, CORES, frames_dev // 2, d_model), bf16),
                pltpu.VMEM((batch, frames_dev, d_model), bf16),
                square, square, square, square, square,
                pltpu.VMEM((d_model, wide), bf16), pltpu.VMEM((wide, d_model), bf16),
                clip_rows, clip_rows,
                pltpu.VMEM((d_model, frames_all), bf16), pltpu.VMEM((frames_all, d_model), bf16),
                pltpu.VMEM((frames_dev, d_model), bf16),
                pltpu.SemaphoreType.DMA((per + 6,)), pltpu.SemaphoreType.DMA((batch,)),
                pltpu.SemaphoreType.DMA((per, KINDS)), pltpu.SemaphoreType.DMA((per, KINDS)),
                pltpu.SemaphoreType.DMA((5, batch)), pltpu.SemaphoreType.DMA((5, batch)),
            ],
            compiler_params=pltpu.CompilerParams(collective_id=0, has_side_effects=True, vmem_limit_bytes=VMEM_BYTES),
            name="encoder",
        )(x_rows, w_query, w_key, w_value, w_out, w_up, w_down, ln1_gain, ln1_bias, b_query, b_value, b_out,
          ln2_gain, ln2_bias, b_up, b_down, lnp_gain, lnp_bias)
        y_all = y_all.reshape(batch, frames_all, d_model)

        ckt = jnp.swapaxes(cross_wk, 1, 2).reshape(layers * width, d_model)
        cvt = jnp.swapaxes(cross_wv, 1, 2).reshape(layers * width, d_model)
        shape = jax.ShapeDtypeStruct((layers, batch, width, frames_all), bf16)
        out_buf = pltpu.VMEM((2, layers, width, frames_all), bf16)
        held = pl.pallas_call(
            cache_kernel,
            in_specs=[hbm, vmem, vmem, vmem],
            out_specs=[hbm, hbm], out_shape=[shape, shape],
            scratch_shapes=[
                pltpu.VMEM((layers * width, 1), jnp.float32), pltpu.VMEM((4, frames_all, d_model), bf16), out_buf, out_buf,
                pltpu.SemaphoreType.DMA((4,)), pltpu.SemaphoreType.DMA((2,)), pltpu.SemaphoreType.DMA((2,)),
            ],
            compiler_params=pltpu.CompilerParams(vmem_limit_bytes=VMEM_BYTES),
            name="caches",
        )(y_all, ckt, cvt, cross_bv)
        heads = width // HEAD_DIM
        return tuple(jnp.moveaxis(buf.reshape(layers, batch, heads, HEAD_DIM, frames_all), 4, 2) for buf in held)

    in_specs = (P('dp', 'sp', None),) + (P(),) * 17 + (P(None, None, 'sp'), P(None, None, 'sp'), P(None, 'sp'))
    out_specs = (P(None, 'dp', None, 'sp', None), P(None, 'dp', None, 'sp', None))
    return jax.shard_map(device_fn, mesh=mesh, in_specs=in_specs, out_specs=out_specs, check_vma=False)
```
